32 devices in a mesh: section: 4 (over x, core), dp: 8 (over z, y).
Axes of the slice: x: 2, y: 2, z: 4, core: 2. Of those that a mesh axis runs over, the one named last changes fastest.
Arguments:
- clean_latent: float32 [64, 256], P('dp'), may hold values from -6 to 6
- noise_draw: float32 [64, 256], P('dp'), may hold values from -6 to 6
- step_index: int32 [64], P('dp'), may hold values from 250 to 1000
- labels: int32 [64], P('dp'), may hold values from 0 to 999
- guide_level: int32 [64], P('dp'), may hold values from 0 to 8
- class_table: bfloat16 [1001, 1152], replicated, may hold values from -6 to 6
- embed_in: bfloat16 [16, 1152], replicated, may hold values from -1.5 to 1.5
- embed_out: bfloat16 [1152, 16], replicated, may hold values from -0.1875 to 0.1875
- teacher_up: bfloat16 [4, 1152, 2304], P('section', 'dp'), may hold values from -0.1875 to 0.1875
- teacher_down: bfloat16 [4, 2304, 1152], P('section', 'dp'), may hold values from -0.125 to 0.125
- teacher_gain: float32 [4, 3, 1152], P('section'), may hold values from -3 to 3
- teacher_bias: float32 [4, 3, 1152], P('section'), may hold values from -3 to 3
- student_up: bfloat16 [1152, 4608], P(None, 'section'), may hold values from -0.1875 to 0.1875
- student_down: bfloat16 [4608, 1152], P('section'), may hold values from -0.09375 to 0.09375
- student_gain: float32 [3, 1152], replicated, may hold values from -3 to 3
- student_bias: float32 [3, 1152], replicated, may hold values from -3 to 3
- guide_vec: float32 [1152], replicated, may hold values from -3 to 3
Outputs:
- distill_target: float32 [64, 256], P('dp')
- grad_up: float32 [1152, 4608], P('dp', 'section')
- grad_down: float32 [4608, 1152], P(('section', 'dp'))
The draws below stay inside these ranges and needn't reach their ends.
All inputs are finite; a program needn't handle non-finite values.
Results may differ from the reference program's by a relative error of at most 0.017.
Values may be sent and summed in bfloat16 or wider, within the bound.
A program may use at most 128 MiB of HBM per device.

```python
import math
import jax
import jax.numpy as jnp
from jax import lax

D = 1152
FF_T = 2304
FF_S = 4608
CLASSES = 1000
CH = 16
TSTEPS = 1000
STRIDE = 125
SEQ = 16
SECTIONS = 4
SAMPLES = 64


def place_ends(entries, rng, least, largest):
    extent = entries.shape
    place = [jax.random.randint(jax.random.fold_in(rng, axis), (), 0, extent[axis]) for axis in range(len(extent))]
    entries = entries.at[tuple(place)].set(least)
    longest = extent.index(max(extent))
    place[longest] = (place[longest] + 1) % extent[longest]
    return entries.at[tuple(place)].set(largest)


def shard_levels(key, shape, pieces, smallest, high):
    factor_of, own = 1.0, jax.random.fold_in(key, 6)
    for axis_at, blocks in pieces:
        steps = jnp.exp(jax.random.uniform(jax.random.fold_in(own, axis_at), (blocks,), jnp.float32, smallest / len(pieces), high / len(pieces)))
        factor_of = factor_of * jnp.repeat(steps, shape[axis_at] // blocks).reshape([-1 if axis == axis_at else 1 for axis in range(len(shape))])
    return factor_of


def gaussian(own_key, shape, scale, reach, shards=(), held_as=jnp.bfloat16):
    entries = jax.random.normal(own_key, shape, jnp.float32) * scale
    if len(shards) > 0:
        entries = shard_levels(own_key, shape, shards, -0.22, 0.18) * entries
    return jnp.clip(entries, min=-reach, max=reach).astype(held_as)


def setup_inputs(seed: int = 0) -> dict:
    seeds = jax.random.split(jax.random.key(seed), 18)
    return {
        "clean_latent": gaussian(seeds[0], (SAMPLES, SEQ * CH), 1.0, 6.0, ((0, 8),), jnp.float32),
        "noise_draw": gaussian(seeds[1], (SAMPLES, SEQ * CH), 1.0, 6.0, ((0, 8),), jnp.float32),
        "step_index": place_ends(jax.random.randint(seeds[2], (SAMPLES,), 2 * STRIDE, TSTEPS + 1), jax.random.fold_in(seeds[2], 1), 2 * STRIDE, TSTEPS).astype(jnp.int32),
        "labels": place_ends(jax.random.randint(seeds[3], (SAMPLES,), 0, CLASSES), jax.random.fold_in(seeds[3], 1), 0, CLASSES - 1).astype(jnp.int32),
        "guide_level": place_ends(jax.random.randint(seeds[4], (SAMPLES,), 0, 9), jax.random.fold_in(seeds[4], 1), 0, 8).astype(jnp.int32),
        "class_table": gaussian(seeds[5], (CLASSES + 1, D), 1.0, 6.0),
        "embed_in": gaussian(seeds[6], (CH, D), CH ** -0.5, 1.5),
        "embed_out": gaussian(seeds[7], (D, CH), D ** -0.5, 0.1875),
        "teacher_up": gaussian(seeds[8], (SECTIONS, D, FF_T), D ** -0.5, 0.1875, ((0, 4), (1, 8))),
        "teacher_down": gaussian(seeds[9], (SECTIONS, FF_T, D), FF_T ** -0.5, 0.125, ((0, 4), (1, 8))),
        "teacher_gain": gaussian(seeds[10], (SECTIONS, 3, D), 0.5, 3.0, ((0, 4),), jnp.float32),
        "teacher_bias": gaussian(seeds[11], (SECTIONS, 3, D), 0.5, 3.0, ((0, 4),), jnp.float32),
        "student_up": gaussian(seeds[12], (D, FF_S), D ** -0.5, 0.1875, ((1, 4),)),
        "student_down": gaussian(seeds[13], (FF_S, D), FF_S ** -0.5, 0.09375, ((0, 4),)),
        "student_gain": gaussian(seeds[14], (3, D), 0.5, 3.0, (), jnp.float32),
        "student_bias": gaussian(seeds[15], (3, D), 0.5, 3.0, (), jnp.float32),
        "guide_vec": gaussian(seeds[16], (D,), 0.5, 3.0, (), jnp.float32),
    }


norm_eps = 1e-06

def layer_norm(values):
    center = values - lax.optimization_barrier(jnp.mean(values, axis=-1, keepdims=True))
    spread = lax.optimization_barrier(jnp.mean(center * center, axis=-1, keepdims=True))
    return center * lax.rsqrt(spread + norm_eps)

def sinusoid(step_ids, model_width):
    half_width = model_width // 2
    frequency = jnp.exp(-math.log(10000.0) * jnp.arange(half_width, dtype=jnp.float32) / half_width)
    phase_arg = step_ids.astype(jnp.float32)[:, None] * frequency[None, :]
    return jnp.concatenate([jnp.cos(phase_arg), jnp.sin(phase_arg)], axis=-1)

def plan(step_ids):
    angle_t = 0.5 * math.pi / TSTEPS * step_ids.astype(jnp.float32)
    return (jnp.cos(angle_t), jnp.sin(angle_t))

def embed_tokens(latent, embed_in):
    leading = latent.shape[0]
    patches = latent.reshape(leading * (latent.shape[1] // CH), CH).astype(jnp.bfloat16)
    tokens = jnp.dot(patches, embed_in, preferred_element_type=jnp.float32)
    return tokens.reshape(leading, latent.shape[1] // CH, embed_in.shape[1]).astype(jnp.bfloat16)

def mlp_block(inputs, modulation, up_proj, down_proj):
    groups, seq_len, model_width = inputs.shape
    residual_in = inputs.astype(jnp.float32)
    shift_rows = modulation[:, 0, None, :]
    scale_rows = modulation[:, 1, None, :]
    gate_rows = modulation[:, 2, None, :]
    normed = (layer_norm(residual_in) * (1.0 + scale_rows) + shift_rows).astype(jnp.bfloat16)
    pre_act = jnp.dot(normed.reshape(groups * seq_len, model_width), up_proj, preferred_element_type=jnp.float32)
    hidden = jax.nn.gelu(pre_act, approximate=True).astype(jnp.bfloat16)
    mixed = jnp.dot(hidden, down_proj, preferred_element_type=jnp.float32).reshape(groups, seq_len, model_width)
    return (residual_in + gate_rows * mixed).astype(jnp.bfloat16)

def velocity(states, embed_out):
    groups, seq_len, model_width = states.shape
    normed = layer_norm(states.astype(jnp.float32)).astype(jnp.bfloat16)
    result = jnp.dot(normed.reshape(groups * seq_len, model_width), embed_out, preferred_element_type=jnp.float32)
    return result.reshape(groups, seq_len * embed_out.shape[1])

def ddim_step(latent, predicted, time_now, time_next):
    alpha_now, sigma_now = plan(time_now)
    alpha_next, sigma_next = plan(time_next)
    clean_est = alpha_now[:, None] * latent - sigma_now[:, None] * predicted
    noise_est = sigma_now[:, None] * latent + alpha_now[:, None] * predicted
    return alpha_next[:, None] * clean_est + sigma_next[:, None] * noise_est

def gelu_slope(pre_act):
    return jax.vjp(lambda inner: jax.nn.gelu(inner, approximate=True), pre_act)[1](jnp.ones_like(pre_act))[0]

def reference(clean_latent, noise_draw, step_index, labels, guide_level, class_table, embed_in, embed_out, teacher_up, teacher_down, teacher_gain, teacher_bias, student_up, student_down, student_gain, student_bias, guide_vec):
    model_width = class_table.shape[1]
    samples = clean_latent.shape[0]
    seq_len = clean_latent.shape[1] // CH
    alpha_t, sigma_t = plan(step_index)
    noised = alpha_t[:, None] * clean_latent + sigma_t[:, None] * noise_draw
    guidance = 0.5 * guide_level.astype(jnp.float32)
    label_rows = jnp.take(class_table, labels, axis=0).astype(jnp.float32)
    null_row = class_table[class_table.shape[0] - 1].astype(jnp.float32)
    first_in = embed_tokens(noised, embed_in)
    latent = noised
    for which_step in range(2):
        time_now = step_index - which_step * STRIDE
        wave_rows = sinusoid(time_now, model_width)
        conditions = jnp.stack([wave_rows + label_rows, wave_rows + null_row[None, :]], axis=1)
        entry_rows = first_in if which_step == 0 else embed_tokens(latent, embed_in)
        states = jnp.stack([entry_rows, entry_rows], axis=1).reshape(samples * 2, seq_len, model_width)
        for layer in range(SECTIONS):
            modulation = conditions[:, :, None, :] * teacher_gain[layer] + teacher_bias[layer]
            states = mlp_block(states, modulation.reshape(samples * 2, 3, model_width), teacher_up[layer], teacher_down[layer])
        predicted = velocity(states, embed_out).reshape(samples, 2, seq_len * CH)
        guided = (1.0 + guidance)[:, None] * predicted[:, 0] - guidance[:, None] * predicted[:, 1]
        latent = ddim_step(latent, guided, time_now, time_now - STRIDE)
    alpha_end, sigma_end = plan(step_index - 2 * STRIDE)
    sigma_ratio = sigma_end / sigma_t
    distill_target = (latent - sigma_ratio[:, None] * noised) / (alpha_end - sigma_ratio * alpha_t)[:, None]
    student_cond = sinusoid(step_index, model_width) + label_rows + guidance[:, None] * guide_vec[None, :]
    modulation = student_cond[:, None, :] * student_gain[None] + student_bias[None]
    shift_rows = modulation[:, 0, None, :]
    scale_rows = modulation[:, 1, None, :]
    gate_rows = modulation[:, 2, None, :]
    row_count = samples * seq_len
    residual_in = first_in.astype(jnp.float32)
    normed = (layer_norm(residual_in) * (1.0 + scale_rows) + shift_rows).astype(jnp.bfloat16).reshape(row_count, model_width)
    pre_act = jnp.dot(normed, student_up, preferred_element_type=jnp.float32)
    hidden = jax.nn.gelu(pre_act, approximate=True).astype(jnp.bfloat16)
    mixed = jnp.dot(hidden, student_down, preferred_element_type=jnp.float32).reshape(samples, seq_len, model_width)
    state_rows = residual_in + gate_rows * mixed
    normed_out, pullback = jax.vjp(layer_norm, state_rows)
    predicted = jnp.dot(normed_out.astype(jnp.bfloat16).reshape(row_count, model_width), embed_out, preferred_element_type=jnp.float32).reshape(samples, seq_len * CH)
    estimate = alpha_t[:, None] * noised - sigma_t[:, None] * predicted
    weight = jnp.maximum(alpha_t * alpha_t / (sigma_t * sigma_t), 1.0)
    element_count = clean_latent.shape[0] * clean_latent.shape[1]
    slope_pred = -2.0 / element_count * (sigma_t * weight)[:, None] * (estimate - distill_target)
    back_norm = jnp.dot(slope_pred.reshape(row_count, CH), embed_out.astype(jnp.float32).T, precision=lax.Precision.HIGHEST)
    back_state = pullback(back_norm.reshape(samples, seq_len, model_width))[0]
    back_part = (gate_rows * back_state).astype(jnp.bfloat16).reshape(row_count, model_width)
    back_hidden = lax.dot_general(back_part, student_down, (((1,), (1,)), ((), ())), preferred_element_type=jnp.float32)
    back_pre = (back_hidden * gelu_slope(pre_act)).astype(jnp.bfloat16)
    grad_up = lax.dot_general(normed, back_pre, (((0,), (0,)), ((), ())), preferred_element_type=jnp.float32)
    grad_down = lax.dot_general(hidden, back_part, (((0,), (0,)), ((), ())), preferred_element_type=jnp.float32)
    return (distill_target, grad_up, grad_down)
```

```python
import math

import jax
import jax.numpy as jnp
from jax import lax
from jax.sharding import PartitionSpec as P

CH = 16
TSTEPS = 1000
STRIDE = 125


norm_eps = 1e-06


def shifted(shard, axis, by):
    length = lax.axis_size(axis)
    return lax.ppermute(shard, axis, [(i, (i + by) % length) for i in range(length)])


def from_root(shard, axis, root):
    mine = lax.axis_index(axis) == root
    return lax.psum(jnp.where(mine, shard, jnp.zeros_like(shard)), axis)


def layer_norm(values):
    center = values - jnp.mean(values, axis=-1, keepdims=True)
    spread = jnp.mean(center * center, axis=-1, keepdims=True)
    return center * lax.rsqrt(spread + norm_eps)


def sinusoid(step_ids, model_width):
    half_width = model_width // 2
    frequency = jnp.exp(-math.log(10000.0) * jnp.arange(half_width, dtype=jnp.float32) / half_width)
    phase_arg = step_ids.astype(jnp.float32)[:, None] * frequency[None, :]
    return jnp.concatenate([jnp.cos(phase_arg), jnp.sin(phase_arg)], axis=-1)


def plan(step_ids):
    angle_t = 0.5 * math.pi / TSTEPS * step_ids.astype(jnp.float32)
    return (jnp.cos(angle_t), jnp.sin(angle_t))


def embed_tokens(latent, embed_in):
    leading = latent.shape[0]
    patches = latent.reshape(leading * (latent.shape[1] // CH), CH).astype(jnp.bfloat16)
    tokens = jnp.dot(patches, embed_in, preferred_element_type=jnp.float32)
    return tokens.reshape(leading, latent.shape[1] // CH, embed_in.shape[1]).astype(jnp.bfloat16)


def mlp_block(inputs, modulation, up_proj, down_proj):
    groups, seq_len, model_width = inputs.shape
    residual_in = inputs.astype(jnp.float32)
    shift_rows = modulation[:, 0, None, :]
    scale_rows = modulation[:, 1, None, :]
    gate_rows = modulation[:, 2, None, :]
    normed = (layer_norm(residual_in) * (1.0 + scale_rows) + shift_rows).astype(jnp.bfloat16)
    pre_act = jnp.dot(
        normed.reshape(groups * seq_len, model_width), up_proj, preferred_element_type=jnp.float32
    )
    hidden = jax.nn.gelu(pre_act, approximate=True).astype(jnp.bfloat16)
    mixed = jnp.dot(hidden, down_proj, preferred_element_type=jnp.float32).reshape(
        groups, seq_len, model_width
    )
    return (residual_in + gate_rows * mixed).astype(jnp.bfloat16)


def velocity(states, embed_out):
    groups, seq_len, model_width = states.shape
    normed = layer_norm(states.astype(jnp.float32)).astype(jnp.bfloat16)
    result = jnp.dot(
        normed.reshape(groups * seq_len, model_width), embed_out, preferred_element_type=jnp.float32
    )
    return result.reshape(groups, seq_len * embed_out.shape[1])


def ddim_step(latent, predicted, time_now, time_next):
    alpha_now, sigma_now = plan(time_now)
    alpha_next, sigma_next = plan(time_next)
    clean_est = alpha_now[:, None] * latent - sigma_now[:, None] * predicted
    noise_est = sigma_now[:, None] * latent + alpha_now[:, None] * predicted
    return alpha_next[:, None] * clean_est + sigma_next[:, None] * noise_est


def gelu_slope(pre_act):
    return jax.vjp(lambda inner: jax.nn.gelu(inner, approximate=True), pre_act)[1](
        jnp.ones_like(pre_act)
    )[0]


def run_chunks(count, one, operands, shared):
    if count == 1:
        return one(operands, *shared)

    def step(carry, piece):
        out = one(piece, *shared)
        return (carry[0] + out[0], carry[1] + out[1]), None

    split = [a.reshape((count, a.shape[0] // count) + a.shape[1:]) for a in operands]
    shapes = jax.eval_shape(one, [a[0] for a in split], *shared)
    zeros = tuple(jnp.zeros(s.shape, s.dtype) for s in shapes)
    return lax.scan(step, zeros, split)[0]


def teacher_chain(first_in, noised, guidance, step_index, mods, up, down, embed_in, embed_out):
    section_count = lax.axis_size("section")
    section_at = lax.axis_index("section")
    micro, seq_len, model_width = first_in.shape

    def paired(tokens):
        return jnp.broadcast_to(tokens[:, None], (micro, 2, seq_len, model_width)).reshape(
            2 * micro, seq_len, model_width
        )

    latent = noised
    states = paired(first_in)
    for which_step in range(2):
        mod = mods[which_step].reshape(2 * micro, 3, model_width)
        if which_step:
            states = paired(embed_tokens(latent, embed_in))
        for layer in range(section_count):
            states = mlp_block(states, mod, up, down)
            if layer < section_count - 1:
                states = lax.ppermute(states, "section", [(layer, layer + 1)])
        predicted = velocity(states, embed_out).reshape(micro, 2, -1)
        weight = guidance[:, None]
        guided = (1.0 + weight) * predicted[:, 0] - weight * predicted[:, 1]
        time_now = step_index - which_step * STRIDE
        stepped = ddim_step(latent, guided, time_now, time_now - STRIDE)
        if which_step == 0:
            returned = lax.ppermute(
                stepped, "section", [(section_count - 1, 0)]
            )
            latent = jnp.where(section_at == section_count - 1, stepped, returned)
    return stepped


def body(
    clean_latent,
    noise_draw,
    step_index,
    labels,
    guide_level,
    class_table,
    embed_in,
    embed_out,
    teacher_up,
    teacher_down,
    teacher_gain,
    teacher_bias,
    student_up,
    student_down,
    student_gain,
    student_bias,
    guide_vec,
):
    section_count = lax.axis_size("section")
    dp_count = lax.axis_size("dp")
    section_at = lax.axis_index("section")
    dp_at = lax.axis_index("dp")
    micro = clean_latent.shape[0]
    width = clean_latent.shape[1]
    seq_len = width // CH
    model_width = class_table.shape[1]
    up = lax.all_gather(teacher_up[0], "dp", axis=0, tiled=True)
    down = lax.all_gather(teacher_down[0], "dp", axis=0, tiled=True)
    alpha_t, sigma_t = plan(step_index)
    noised = alpha_t[:, None] * clean_latent + sigma_t[:, None] * noise_draw
    guidance = 0.5 * guide_level.astype(jnp.float32)
    label_rows = jnp.take(class_table, labels, axis=0).astype(jnp.float32)
    null_row = class_table[class_table.shape[0] - 1].astype(jnp.float32)
    wave_rows = jnp.stack(
        [sinusoid(step_index - step_k * STRIDE, model_width) for step_k in range(2)]
    )
    conditions = jnp.stack(
        [wave_rows + label_rows[None], wave_rows + null_row[None, None, :]], axis=2
    )
    mods = (
        conditions[:, :, :, None, :] * teacher_gain[0][None, None, None]
        + teacher_bias[0][None, None, None]
    )
    first_in = embed_tokens(noised, embed_in)
    ending = teacher_chain(
        first_in, noised, guidance, step_index, mods, up, down, embed_in, embed_out
    )
    alpha_end, sigma_end = plan(step_index - 2 * STRIDE)
    sigma_ratio = sigma_end / sigma_t
    goal_latent = (ending - sigma_ratio[:, None] * noised) / (alpha_end - sigma_ratio * alpha_t)[
        :, None
    ]

    packed = jnp.concatenate(
        [
            noised,
            step_index.astype(jnp.float32)[:, None],
            labels.astype(jnp.float32)[:, None],
            guide_level.astype(jnp.float32)[:, None],
        ],
        axis=1,
    )
    packed = lax.all_gather(packed, "dp", axis=0, tiled=True)
    all_noised = packed[:, :width]
    all_steps = packed[:, width].astype(jnp.int32)
    all_labels = packed[:, width + 1].astype(jnp.int32)
    all_guidance = 0.5 * packed[:, width + 2]

    def student_front(noised, steps, labels, guidance, student_up):
        rows = noised.shape[0] * seq_len
        label_rows = jnp.take(class_table, labels, axis=0).astype(jnp.float32)
        cond = sinusoid(steps, model_width) + label_rows + guidance[:, None] * guide_vec[None, :]
        modulation = cond[:, None, :] * student_gain[None] + student_bias[None]
        residual_in = embed_tokens(noised, embed_in).astype(jnp.float32)
        normed = (
            (layer_norm(residual_in) * (1.0 + modulation[:, 1, None, :]) + modulation[:, 0, None, :])
            .astype(jnp.bfloat16)
            .reshape(rows, model_width)
        )
        pre_act = jnp.dot(normed, student_up, preferred_element_type=jnp.float32)
        hidden = jax.nn.gelu(pre_act, approximate=True).astype(jnp.bfloat16)
        return residual_in, modulation[:, 2, None, :], normed, pre_act, hidden

    own = student_front(noised, step_index, labels, guidance, student_up)
    partial_value = jnp.dot(own[4], student_down, preferred_element_type=jnp.float32)
    mixed = lax.psum(partial_value.astype(jnp.bfloat16), "section")
    all_mixed = lax.all_gather(mixed, "dp", axis=0, tiled=True)
    all_mixed = all_mixed.reshape(micro * dp_count, seq_len, model_width)

    total = micro * dp_count
    element_count = total * width
    up_share = model_width // dp_count
    down_share = student_down.shape[0] // dp_count

    mine = section_at == section_count - 1
    gathered = lax.all_gather(goal_latent, ("section", "dp"), axis=0, tiled=True)
    all_target = gathered[total * (section_count - 1):]
    distill_target = lax.dynamic_slice_in_dim(all_target, dp_at * micro, micro, 0)

    def student_grads(operands, student_up, student_down):
        noised, steps, labels, guidance, mixed, target = operands
        count = noised.shape[0]
        rows = count * seq_len
        residual_in, gate_rows, normed, pre_act, hidden = student_front(
            noised, steps, labels, guidance, student_up
        )
        state_rows = residual_in + gate_rows * mixed.astype(jnp.float32)
        alpha_t, sigma_t = plan(steps)
        normed_out, pullback = jax.vjp(layer_norm, state_rows)
        predicted = jnp.dot(
            normed_out.astype(jnp.bfloat16).reshape(rows, model_width),
            embed_out,
            preferred_element_type=jnp.float32,
        ).reshape(count, width)
        estimate = alpha_t[:, None] * noised - sigma_t[:, None] * predicted
        weight = jnp.maximum(alpha_t * alpha_t / (sigma_t * sigma_t), 1.0)
        slope_pred = -2.0 / element_count * (sigma_t * weight)[:, None] * (estimate - target)
        back_norm = jnp.dot(
            slope_pred.reshape(rows, CH),
            embed_out.astype(jnp.float32).T,
            precision=lax.Precision.HIGHEST,
        )
        back_state = pullback(back_norm.reshape(count, seq_len, model_width))[0]
        back_part = (gate_rows * back_state).astype(jnp.bfloat16).reshape(rows, model_width)
        back_hidden = lax.dot_general(
            back_part, student_down, (((1,), (1,)), ((), ())), preferred_element_type=jnp.float32
        )
        back_pre = (back_hidden * gelu_slope(pre_act)).astype(jnp.bfloat16)
        normed_share = lax.dynamic_slice_in_dim(normed, dp_at * up_share, up_share, 1)
        hidden_share = lax.dynamic_slice_in_dim(hidden, dp_at * down_share, down_share, 1)
        contract_rows = (((0,), (0,)), ((), ()))
        return (
            lax.dot_general(
                normed_share, back_pre, contract_rows, preferred_element_type=jnp.float32
            ),
            lax.dot_general(
                hidden_share, back_part, contract_rows, preferred_element_type=jnp.float32
            ),
        )

    operands = [all_noised, all_steps, all_labels, all_guidance, all_mixed, all_target]
    grad_up, grad_down = run_chunks(
        max(1, dp_count // 8), student_grads, operands, (student_up, student_down)
    )
    return (distill_target, grad_up, grad_down)


def solution(mesh):
    return jax.shard_map(
        body,
        mesh=mesh,
        in_specs=(
            P("dp", None),
            P("dp", None),
            P("dp"),
            P("dp"),
            P("dp"),
            P(),
            P(),
            P(),
            P("section", "dp", None),
            P("section", "dp", None),
            P("section", None, None),
            P("section", None, None),
            P(None, "section"),
            P("section", None),
            P(),
            P(),
            P(),
        ),
        out_specs=(P("dp", None), P("dp", "section"), P(("section", "dp"), None)),
        check_vma=False,
    )
```

```python
import functools
import math

import jax
import jax.numpy as jnp
from jax import lax
from jax.experimental import pallas as pl
from jax.experimental.pallas import tpu as pltpu
from jax.sharding import PartitionSpec as P

CH = 16
TSTEPS = 1000
STRIDE = 125


norm_eps = 1e-06


def shifted(shard, axis, by):
    length = lax.axis_size(axis)
    return lax.ppermute(shard, axis, [(i, (i + by) % length) for i in range(length)])


def from_root(shard, axis, root):
    mine = lax.axis_index(axis) == root
    return lax.psum(jnp.where(mine, shard, jnp.zeros_like(shard)), axis)


def layer_norm(values):
    center = values - jnp.mean(values, axis=-1, keepdims=True)
    spread = jnp.mean(center * center, axis=-1, keepdims=True)
    return center * lax.rsqrt(spread + norm_eps)


def sinusoid(step_ids, model_width):
    half_width = model_width // 2
    frequency = jnp.exp(-math.log(10000.0) * jnp.arange(half_width, dtype=jnp.float32) / half_width)
    phase_arg = step_ids.astype(jnp.float32)[:, None] * frequency[None, :]
    return jnp.concatenate([jnp.cos(phase_arg), jnp.sin(phase_arg)], axis=-1)


def plan(step_ids):
    angle_t = 0.5 * math.pi / TSTEPS * step_ids.astype(jnp.float32)
    return (jnp.cos(angle_t), jnp.sin(angle_t))


def embed_tokens(latent, embed_in):
    leading = latent.shape[0]
    patches = latent.reshape(leading * (latent.shape[1] // CH), CH).astype(jnp.bfloat16)
    tokens = jnp.dot(patches, embed_in, preferred_element_type=jnp.float32)
    return tokens.reshape(leading, latent.shape[1] // CH, embed_in.shape[1]).astype(jnp.bfloat16)


def mlp_block(inputs, modulation, up_proj, down_proj):
    groups, seq_len, model_width = inputs.shape
    residual_in = inputs.astype(jnp.float32)
    shift_rows = modulation[:, 0, None, :]
    scale_rows = modulation[:, 1, None, :]
    gate_rows = modulation[:, 2, None, :]
    normed = (layer_norm(residual_in) * (1.0 + scale_rows) + shift_rows).astype(jnp.bfloat16)
    pre_act = jnp.dot(
        normed.reshape(groups * seq_len, model_width), up_proj, preferred_element_type=jnp.float32
    )
    hidden = jax.nn.gelu(pre_act, approximate=True).astype(jnp.bfloat16)
    mixed = jnp.dot(hidden, down_proj, preferred_element_type=jnp.float32).reshape(
        groups, seq_len, model_width
    )
    return (residual_in + gate_rows * mixed).astype(jnp.bfloat16)


def velocity(states, embed_out):
    groups, seq_len, model_width = states.shape
    normed = layer_norm(states.astype(jnp.float32)).astype(jnp.bfloat16)
    result = jnp.dot(
        normed.reshape(groups * seq_len, model_width), embed_out, preferred_element_type=jnp.float32
    )
    return result.reshape(groups, seq_len * embed_out.shape[1])


def ddim_step(latent, predicted, time_now, time_next):
    alpha_now, sigma_now = plan(time_now)
    alpha_next, sigma_next = plan(time_next)
    clean_est = alpha_now[:, None] * latent - sigma_now[:, None] * predicted
    noise_est = sigma_now[:, None] * latent + alpha_now[:, None] * predicted
    return alpha_next[:, None] * clean_est + sigma_next[:, None] * noise_est


def gelu_slope(pre_act):
    return jax.vjp(lambda inner: jax.nn.gelu(inner, approximate=True), pre_act)[1](
        jnp.ones_like(pre_act)
    )[0]


def run_chunks(count, one, operands, shared):
    if count == 1:
        return one(operands, *shared)

    def step(carry, piece):
        out = one(piece, *shared)
        return (carry[0] + out[0], carry[1] + out[1]), None

    split = [a.reshape((count, a.shape[0] // count) + a.shape[1:]) for a in operands]
    shapes = jax.eval_shape(one, [a[0] for a in split], *shared)
    zeros = tuple(jnp.zeros(s.shape, s.dtype) for s in shapes)
    return lax.scan(step, zeros, split)[0]


def teacher_chain(first_in, noised, guidance, step_index, mods, up, down, embed_in, embed_out):
    section_count = lax.axis_size("section")
    section_at = lax.axis_index("section")
    micro, seq_len, model_width = first_in.shape

    def paired(tokens):
        return jnp.broadcast_to(tokens[:, None], (micro, 2, seq_len, model_width)).reshape(
            2 * micro, seq_len, model_width
        )

    latent = noised
    states = paired(first_in)
    for which_step in range(2):
        mod = mods[which_step].reshape(2 * micro, 3, model_width)
        if which_step:
            states = paired(embed_tokens(latent, embed_in))
        for layer in range(section_count):
            states = mlp_block(states, mod, up, down)
            if layer < section_count - 1:
                states = lax.ppermute(states, "section", [(layer, layer + 1)])
        predicted = velocity(states, embed_out).reshape(micro, 2, -1)
        weight = guidance[:, None]
        guided = (1.0 + weight) * predicted[:, 0] - weight * predicted[:, 1]
        time_now = step_index - which_step * STRIDE
        stepped = ddim_step(latent, guided, time_now, time_now - STRIDE)
        if which_step == 0:
            returned = lax.ppermute(
                stepped, "section", [(section_count - 1, 0)]
            )
            latent = jnp.where(section_at == section_count - 1, stepped, returned)
    return stepped


def chunked_mlp(normed, up_ref, down_ref, width):
    def piece(j, total):
        at = pl.ds(pl.multiple_of(j * width, width), width)
        hidden = jax.nn.gelu(
            jnp.dot(normed, up_ref[:, at], preferred_element_type=jnp.float32), approximate=True
        ).astype(jnp.bfloat16)
        return total + jnp.dot(hidden, down_ref[at, :], preferred_element_type=jnp.float32)

    zero = jnp.zeros((normed.shape[0], down_ref.shape[1]), jnp.float32)
    return lax.fori_loop(0, up_ref.shape[1] // width, piece, zero)


def teacher_kernel(
    dims,
    up_shard, down_shard, packed_in, normed_own, stud_up, stud_down,
    mods, first_in, latent_in, coef, embed_in, embed_out,
    packed_all, mixed_all, target_all,
    up, down, parts, states, outs, velo, z_sem_buf, z_in,
    send, recv,
):
    section_count, dp_count, micro, seq_len = dims
    sec = lax.axis_index("section")
    me = lax.axis_index("dp")
    planes = dp_count // 2
    z, y = me // 2, me % 2
    z_up = lax.rem(z + 1, planes)
    z_dn = lax.rem(z + planes - 1, planes)
    z_op = lax.rem(z + 2, planes)
    tail = section_count - 1

    def at(zz, yy):
        return zz * 2 + yy

    peer, above, below = at(z, 1 - y), at(z_up, y), at(z_dn, y)
    barrier = pltpu.get_barrier_semaphore()
    for k in range(1, dp_count):
        pl.semaphore_signal(
            barrier, inc=1, device_id={"dp": lax.rem(me + k, dp_count)},
            device_id_type=pl.DeviceIdType.MESH,
        )
    for k in range(1, section_count):
        pl.semaphore_signal(
            barrier, inc=1, device_id={"section": lax.rem(sec + k, section_count)},
            device_id_type=pl.DeviceIdType.MESH,
        )
    pl.semaphore_wait(barrier, dp_count + section_count - 2)

    count = [0]

    def copy(src, dst, **device):
        i = count[0]
        count[0] += 1
        return pltpu.make_async_remote_copy(
            src_ref=src, dst_ref=dst, send_sem=send.at[i], recv_sem=recv.at[i],
            device_id=device, device_id_type=pl.DeviceIdType.MESH,
        )

    ur, dr = up_shard.shape[0], down_shard.shape[0]
    ua = (ur // 32) * 16 + 16 * ((ur // 16) % 2)
    da = (dr // 32) * 16

    def rows(ref, size, who, lo=0, n=None):
        n = size if n is None else n
        return ref.at[pl.ds(pl.multiple_of(who * size + lo, 16), n)]

    u, w = functools.partial(rows, up, ur), functools.partial(rows, down, dr)

    def go(c):
        c.start()
        return c

    sent = []

    def ship(src, dst, **device):
        c = go(copy(src, dst, **device))
        sent.append(c)
        return c

    own_slot_rows = micro * seq_len
    packs = []
    for k in range(1, dp_count):
        packs.append(
            ship(packed_in, packed_all.at[me], dp=lax.rem(me + k, dp_count))
        )
    u_up = ship(up_shard, u(me), dp=above)
    u_dn = ship(up_shard, u(me), dp=below)
    w_y = ship(down_shard, w(me), dp=peer)
    w_up = ship(down_shard, w(me), dp=above)
    w_dn = ship(down_shard, w(me), dp=below)
    u_y = ship(up_shard, u(me), dp=peer)
    packed_all[me] = packed_in[...]
    up[pl.ds(pl.multiple_of(me * ur, 16), ur)] = up_shard[...]
    down[pl.ds(pl.multiple_of(me * dr, 16), dr)] = down_shard[...]

    parts[sec] = chunked_mlp(normed_own[...], stud_up, stud_down, 384).astype(jnp.bfloat16)
    part_copies = [
        ship(parts.at[sec], parts.at[sec], section=lax.rem(sec + k, section_count))
        for k in range(1, section_count)
    ]

    u_up.wait_recv()
    f_uu = ship(u(below, 0, ua), u(below, 0, ua), dp=above)
    f_uy1 = ship(u(below), u(below), dp=peer)
    u_dn.wait_recv()
    f_ud = ship(u(above, ua, ur - ua), u(above, ua, ur - ua), dp=below)
    f_uy2 = ship(u(above), u(above), dp=peer)
    w_y.wait_recv()
    v_up = ship(w(peer), w(peer), dp=above)
    v_dn = ship(w(peer), w(peer), dp=below)
    w_up.wait_recv()
    f_wu = ship(w(below, 0, da), w(below, 0, da), dp=above)
    w_dn.wait_recv()
    f_wd = ship(w(above, da, dr - da), w(above, da, dr - da), dp=below)
    f_uu.wait_recv()
    f_ud.wait_recv()
    opp = at(z_op, y)
    f_uy3 = ship(u(opp), u(opp), dp=peer)
    v_up.wait_recv()
    pb = at(z_dn, 1 - y)
    g_wu = ship(w(pb, 0, da), w(pb, 0, da), dp=above)
    v_dn.wait_recv()
    pa = at(z_up, 1 - y)
    g_wd = ship(w(pa, da, dr - da), w(pa, da, dr - da), dp=below)

    for c in part_copies:
        c.wait_recv()
    total = parts[0].astype(jnp.float32)
    for k in range(1, section_count):
        total = total + parts[k].astype(jnp.float32)
    mixed_all[me] = total.astype(jnp.bfloat16)
    for c in (u_y, f_wu, f_wd, f_uy1, f_uy2, f_uy3, g_wu, g_wd):
        c.wait_recv()
    mix_copies = [
        ship(mixed_all.at[me], mixed_all.at[me], dp=lax.rem(me + k, dp_count))
        for k in range(1, dp_count)
    ]

    width = first_in.shape[1]
    nxt = lax.rem(sec + 1, section_count)
    moves = [copy(outs.at[i], states.at[i], section=nxt) for i in range(4)]
    z_move = copy(z_sem_buf, z_in, section=0)
    goal_copies = [
        copy(target_all.at[me], target_all.at[me], dp=lax.rem(me + k, dp_count))
        for k in range(1, dp_count)
    ]
    final_copies = [
        copy(target_all, target_all, section=k) for k in range(tail)
    ]

    for step in range(2):
        if step == 1:
            @pl.when(sec == 0)
            def _():
                z_move.wait_recv()

        for half in range(2):
            slot = 2 * step + half

            @pl.when(sec == 0)
            def _():
                if step == 0:
                    states[slot] = first_in[...]
                else:
                    states[slot] = lax.dot_general(
                        z_in[...].astype(jnp.bfloat16), embed_in[...], (((0,), (0,)), ((), ())),
                        preferred_element_type=jnp.float32,
                    ).astype(jnp.bfloat16)

            @pl.when(sec > 0)
            def _():
                moves[slot].wait_recv()

            residual = states[slot].astype(jnp.float32)
            shift = mods[step, half, 0][:, None, :]
            scale = mods[step, half, 1][:, None, :]
            gate = mods[step, half, 2][:, None, :]
            cube = layer_norm(residual).reshape(micro, seq_len, width)
            normed = (cube * (1.0 + scale) + shift).astype(jnp.bfloat16)
            mixed = chunked_mlp(normed.reshape(micro * seq_len, width), up, down, 768)
            out = residual.reshape(micro, seq_len, width) + gate * mixed.reshape(
                micro, seq_len, width
            )
            outs[slot] = out.reshape(micro * seq_len, width).astype(jnp.bfloat16)

            @pl.when(sec < tail)
            def _():
                moves[slot].start()

            @pl.when(sec == tail)
            def _():
                last = layer_norm(outs[slot].astype(jnp.float32)).astype(jnp.bfloat16)
                velo[half] = lax.dot_general(
                    embed_out[...], last, (((0,), (1,)), ((), ())),
                    preferred_element_type=jnp.float32,
                )

        @pl.when(sec == tail)
        def _():
            level = coef[4:5, :]
            guided = (1.0 + level) * velo[0] - level * velo[1]
            before = latent_in[...] if step == 0 else z_sem_buf[...]
            after = coef[2 * step : 2 * step + 1, :] * before + coef[
                2 * step + 1 : 2 * step + 2, :
            ] * guided
            if step == 0:
                z_sem_buf[...] = after
                z_move.start()
                z_move.wait_send()
            else:
                target_all[me] = coef[5:6, :] * after + coef[6:7, :] * latent_in[...]

    @pl.when(sec == tail)
    def _():
        for c in goal_copies:
            c.start()
        for c in goal_copies:
            c.wait()
        for c in final_copies:
            c.start()
        for c in final_copies:
            c.wait_send()

    for k in range(tail):
        @pl.when(sec == k)
        def _():
            final_copies[k].wait_recv()

    @pl.when(sec < tail)
    def _():
        for c in moves:
            c.wait_send()

    for c in packs + mix_copies:
        c.wait_recv()
    for c in sent:
        c.wait_send()


def teacher_call(dims, operands):
    section_count, dp_count, micro, seq_len = dims
    up_shard, down_shard = operands[0], operands[1]
    width = up_shard.shape[1]
    model_width = down_shard.shape[1]
    row_count = micro * seq_len
    copies = 3 * (dp_count - 1) + 2 * section_count + 64
    block = (row_count, model_width)
    vmem = pl.BlockSpec(memory_space=pltpu.VMEM)
    return pl.pallas_call(
        functools.partial(teacher_kernel, dims),
        out_shape=(
            jax.ShapeDtypeStruct((dp_count,) + operands[2].shape, jnp.float32),
            jax.ShapeDtypeStruct((dp_count,) + block, jnp.bfloat16),
            jax.ShapeDtypeStruct((dp_count, CH, row_count), jnp.float32),
        ),
        in_specs=[vmem] * len(operands),
        out_specs=(vmem,) * 3,
        scratch_shapes=[
            pltpu.VMEM((up_shard.shape[0] * dp_count, width), jnp.bfloat16),
            pltpu.VMEM((down_shard.shape[0] * dp_count, model_width), jnp.bfloat16),
            pltpu.VMEM((section_count,) + block, jnp.bfloat16),
            pltpu.VMEM((4,) + block, jnp.bfloat16),
            pltpu.VMEM((4,) + block, jnp.bfloat16),
            pltpu.VMEM((2, CH, row_count), jnp.float32),
            pltpu.VMEM((CH, row_count), jnp.float32),
            pltpu.VMEM((CH, row_count), jnp.float32),
            pltpu.SemaphoreType.DMA((copies,)),
            pltpu.SemaphoreType.DMA((copies,)),
        ],
        compiler_params=pltpu.CompilerParams(
            collective_id=0, has_side_effects=True, vmem_limit_bytes=56 << 20
        ),
    )(*operands)


def body(
    clean_latent,
    noise_draw,
    step_index,
    labels,
    guide_level,
    class_table,
    embed_in,
    embed_out,
    teacher_up,
    teacher_down,
    teacher_gain,
    teacher_bias,
    student_up,
    student_down,
    student_gain,
    student_bias,
    guide_vec,
):
    section_count = lax.axis_size("section")
    dp_count = lax.axis_size("dp")
    section_at = lax.axis_index("section")
    dp_at = lax.axis_index("dp")
    micro = clean_latent.shape[0]
    width = clean_latent.shape[1]
    seq_len = width // CH
    model_width = class_table.shape[1]
    fused = (
        dp_count == 8
        and section_count == 4
        and teacher_up.shape[1] % 16 == 0
        and teacher_down.shape[1] % 32 == 0
    )
    alpha_t, sigma_t = plan(step_index)
    noised = alpha_t[:, None] * clean_latent + sigma_t[:, None] * noise_draw
    guidance = 0.5 * guide_level.astype(jnp.float32)
    label_rows = jnp.take(class_table, labels, axis=0).astype(jnp.float32)
    null_row = class_table[class_table.shape[0] - 1].astype(jnp.float32)
    wave_rows = jnp.stack(
        [sinusoid(step_index - step_k * STRIDE, model_width) for step_k in range(2)]
    )
    conditions = jnp.stack(
        [wave_rows + label_rows[None], wave_rows + null_row[None, None, :]], axis=2
    )
    mods = (
        conditions[:, :, :, None, :] * teacher_gain[0][None, None, None]
        + teacher_bias[0][None, None, None]
    )
    first_in = embed_tokens(noised, embed_in)
    alpha_end, sigma_end = plan(step_index - 2 * STRIDE)
    sigma_ratio = sigma_end / sigma_t
    packed = jnp.concatenate(
        [
            noised,
            step_index.astype(jnp.float32)[:, None],
            labels.astype(jnp.float32)[:, None],
            guide_level.astype(jnp.float32)[:, None],
        ],
        axis=1,
    )
    def student_normed(noised, steps, labels, guidance):
        rows = noised.shape[0] * seq_len
        label_rows = jnp.take(class_table, labels, axis=0).astype(jnp.float32)
        cond = sinusoid(steps, model_width) + label_rows + guidance[:, None] * guide_vec[None, :]
        modulation = cond[:, None, :] * student_gain[None] + student_bias[None]
        residual_in = embed_tokens(noised, embed_in).astype(jnp.float32)
        normed = (
            (layer_norm(residual_in) * (1.0 + modulation[:, 1, None, :]) + modulation[:, 0, None, :])
            .astype(jnp.bfloat16)
            .reshape(rows, model_width)
        )
        return residual_in, modulation[:, 2, None, :], normed

    def student_front(noised, steps, labels, guidance, student_up):
        residual_in, gate_rows, normed = student_normed(noised, steps, labels, guidance)
        pre_act = jnp.dot(normed, student_up, preferred_element_type=jnp.float32)
        hidden = jax.nn.gelu(pre_act, approximate=True).astype(jnp.bfloat16)
        return residual_in, gate_rows, normed, pre_act, hidden

    total = micro * dp_count
    element_count = total * width
    up_share = model_width // dp_count
    down_share = student_down.shape[0] // dp_count

    goal_scale = 1.0 / (alpha_end - sigma_ratio * alpha_t)
    if fused:
        own_normed = student_normed(noised, step_index, labels, guidance)[2]
        pack_pad = -packed.shape[1] % 128
        packed = jnp.pad(packed, ((0, 0), (0, pack_pad)))
        coefs = []
        for step_k in range(2):
            alpha_k, sigma_k = plan(step_index - step_k * STRIDE)
            alpha_n, sigma_n = plan(step_index - (step_k + 1) * STRIDE)
            coefs += [alpha_n * alpha_k + sigma_n * sigma_k, sigma_n * alpha_k - alpha_n * sigma_k]
        coefs += [guidance, goal_scale, -sigma_ratio * goal_scale, guidance]
        coefs = jnp.repeat(jnp.stack(coefs), seq_len, axis=1)
        packed, all_mixed, all_target = teacher_call(
            (section_count, dp_count, micro, seq_len),
            (
                teacher_up[0],
                teacher_down[0],
                packed,
                own_normed,
                student_up,
                student_down,
                mods.transpose(0, 2, 3, 1, 4),
                first_in.reshape(micro * seq_len, model_width),
                noised.reshape(micro * seq_len, CH).T,
                coefs,
                embed_in,
                embed_out,
            ),
        )
        packed = packed.reshape(total, packed.shape[-1])
        all_target = all_target.transpose(0, 2, 1).reshape(total, width)
    else:
        up = lax.all_gather(teacher_up[0], "dp", axis=0, tiled=True)
        down = lax.all_gather(teacher_down[0], "dp", axis=0, tiled=True)
        ending = teacher_chain(
            first_in, noised, guidance, step_index, mods, up, down, embed_in, embed_out
        )
        goal_latent = (ending - sigma_ratio[:, None] * noised) * goal_scale[:, None]
        packed = lax.all_gather(packed, "dp", axis=0, tiled=True)
        own = student_front(noised, step_index, labels, guidance, student_up)
        partial_value = jnp.dot(own[4], student_down, preferred_element_type=jnp.float32)
        mixed = lax.psum(partial_value.astype(jnp.bfloat16), "section")
        all_mixed = lax.all_gather(mixed, "dp", axis=0, tiled=True)
        gathered = lax.all_gather(goal_latent, ("section", "dp"), axis=0, tiled=True)
        all_target = gathered[total * (section_count - 1):]
    all_mixed = all_mixed.reshape(total, seq_len, model_width)
    all_noised = packed[:, :width]
    all_steps = packed[:, width].astype(jnp.int32)
    all_labels = packed[:, width + 1].astype(jnp.int32)
    all_guidance = 0.5 * packed[:, width + 2]
    distill_target = lax.dynamic_slice_in_dim(all_target, dp_at * micro, micro, 0)

    def student_grads(operands, student_up, student_down):
        noised, steps, labels, guidance, mixed, target = operands
        count = noised.shape[0]
        rows = count * seq_len
        residual_in, gate_rows, normed, pre_act, hidden = student_front(
            noised, steps, labels, guidance, student_up
        )
        state_rows = residual_in + gate_rows * mixed.astype(jnp.float32)
        alpha_t, sigma_t = plan(steps)
        normed_out, pullback = jax.vjp(layer_norm, state_rows)
        predicted = jnp.dot(
            normed_out.astype(jnp.bfloat16).reshape(rows, model_width),
            embed_out,
            preferred_element_type=jnp.float32,
        ).reshape(count, width)
        estimate = alpha_t[:, None] * noised - sigma_t[:, None] * predicted
        weight = jnp.maximum(alpha_t * alpha_t / (sigma_t * sigma_t), 1.0)
        slope_pred = -2.0 / element_count * (sigma_t * weight)[:, None] * (estimate - target)
        back_norm = jnp.dot(
            slope_pred.reshape(rows, CH),
            embed_out.astype(jnp.float32).T,
            precision=lax.Precision.HIGHEST,
        )
        back_state = pullback(back_norm.reshape(count, seq_len, model_width))[0]
        back_part = (gate_rows * back_state).astype(jnp.bfloat16).reshape(rows, model_width)
        back_hidden = lax.dot_general(
            back_part, student_down, (((1,), (1,)), ((), ())), preferred_element_type=jnp.float32
        )
        back_pre = (back_hidden * gelu_slope(pre_act)).astype(jnp.bfloat16)
        normed_share = lax.dynamic_slice_in_dim(normed, dp_at * up_share, up_share, 1)
        hidden_share = lax.dynamic_slice_in_dim(hidden, dp_at * down_share, down_share, 1)
        contract_rows = (((0,), (0,)), ((), ()))
        return (
            lax.dot_general(
                normed_share, back_pre, contract_rows, preferred_element_type=jnp.float32
            ),
            lax.dot_general(
                hidden_share, back_part, contract_rows, preferred_element_type=jnp.float32
            ),
        )

    operands = [all_noised, all_steps, all_labels, all_guidance, all_mixed, all_target]
    grad_up, grad_down = run_chunks(
        max(1, dp_count // 8), student_grads, operands, (student_up, student_down)
    )
    return (distill_target, grad_up, grad_down)


def solution(mesh):
    return jax.shard_map(
        body,
        mesh=mesh,
        in_specs=(
            P("dp", None),
            P("dp", None),
            P("dp"),
            P("dp"),
            P("dp"),
            P(),
            P(),
            P(),
            P("section", "dp", None),
            P("section", "dp", None),
            P("section", None, None),
            P("section", None, None),
            P(None, "section"),
            P("section", None),
            P(),
            P(),
            P(),
        ),
        out_specs=(P("dp", None), P("dp", "section"), P(("section", "dp"), None)),
        check_vma=False,
    )
```
